128 devices in a mesh: row: 8 (over y, core), col: 16 (over z, x).
Axes of the slice: x: 4, y: 4, z: 4, core: 2. Of those that a mesh axis runs over, the one named last changes fastest.
Arguments:
- left_derivatives: bfloat16 [1024, 512, 512], P(('row', 'col')), may hold values from -0.25 to 0.25
- right_derivatives: bfloat16 [1024, 512, 512], P(('row', 'col')), may hold values from -0.25 to 0.25
- bundle_tile_slot: int32 [1024], P(('row', 'col')), may hold values from 0 to 2047, as said below
- tile_pos: int32 [8, 16, 16], P('row', 'col'), may hold values from 0 to 2047, as said below
- right_sides: float32 [16, 262144], P(None, ('row', 'col')), may hold values from -6 to 6
- diagonal: float32 [262144], P(('row', 'col')), may hold values from 0.8 to 3
Outputs:
- solution: float32 [16, 262144], P(None, ('row', 'col'))
The draws below stay inside these ranges and needn't reach their ends.
Inputs may be any that keep to these rules, and one draw needn't show every extreme that they name: `bundle_tile_slot`: bundle b lies on the device of index b // 8 along row+col. The slot g that it names belongs to a device of the same row index. Of the bundles of one device, at most 2 name slots of any one device, and in each row some device is named exactly 2 times by the bundles of every device of that row. `tile_pos`: the 16 entries of one device are distinct.
All inputs are finite; a program needn't handle non-finite values.
Results may differ from the reference program's by a relative error of at most 0.002.
Values may be sent and summed in bfloat16 or wider, within the bound.
No kernel may reach another device: no remote copies, remote signals or barrier semaphores. Data moves between devices by JAX's collectives and lax.ppermute only.
A program may use at most 192 MiB of HBM per device.

```python
import math
import jax
import jax.numpy as jnp
from jax import lax

BLOCK_PARAMS = 512
MEASURE_ROWS = 512
NRHS = 16
BLK_DEV = 4
CAP = 16
SEND_CAP = 2
ITERS = 3
BUN_DEV = 8
BLOCKS = 512
ORDER = 262144
BUNDLE_TOTAL = 1024
N_ROW = 8
N_COL = 16


def slot_counts(key):
    lowest = CAP - CAP // 2
    return jax.random.randint(jax.random.fold_in(key, 101), (N_ROW * N_COL,), lowest, CAP + 1)


def draw_tile_pos(key, part):
    devices = N_ROW * N_COL
    positions = devices * BLK_DEV * BLK_DEV
    device_keys = jax.random.split(jax.random.fold_in(key, 7), devices)

    def choose(device_key):
        return jax.random.permutation(device_key, positions)[:CAP]
    picked = jax.vmap(choose)(device_keys)
    return picked.reshape(N_ROW, N_COL, CAP).astype(jnp.int32)


def draw_bundle_tile_slot(key, part):
    devices = N_ROW * N_COL
    counts = slot_counts(key)
    hottest = jax.random.randint(jax.random.fold_in(key, 103), (N_ROW,), 0, N_COL)
    device_keys = jax.random.split(jax.random.fold_in(key, 107), devices)
    candidates = SEND_CAP * N_COL
    column_of = jnp.arange(candidates, dtype=jnp.int32) // SEND_CAP

    def one_device(device, device_key):
        band_row = device // N_COL
        key_order, key_shuffle, key_slot = jax.random.split(device_key, 3)
        ranking = jax.random.permutation(key_order, candidates).astype(jnp.int32)
        ranking = jnp.where(column_of == hottest[band_row], ranking - candidates, ranking)
        bundle_ordering = jnp.argsort(ranking, stable=True)
        targets = column_of[bundle_ordering[:BUN_DEV]]
        targets = targets[jax.random.permutation(key_shuffle, BUN_DEV)]
        owners = band_row * N_COL + targets
        within = jax.random.randint(key_slot, (BUN_DEV,), 0, counts[owners])
        return owners * CAP + within
    bundle_ids = jax.vmap(one_device)(jnp.arange(devices, dtype=jnp.int32), device_keys)
    return bundle_ids.reshape(-1).astype(jnp.int32)


def steps_of(stream_key, extent, pieces, low, largest):
    factor_of, own = 1.0, jax.random.fold_in(stream_key, 6)
    for axis_at, shards_of in pieces:
        heights = jnp.exp(jax.random.uniform(jax.random.fold_in(own, axis_at), (shards_of,), jnp.float32, low / len(pieces), largest / len(pieces)))
        factor_of = factor_of * jnp.repeat(heights, extent[axis_at] // shards_of).reshape([-1 if axis == axis_at else 1 for axis in range(len(extent))])
    return factor_of


def normal_values(stream_key, shape, deviation, reach, pieces=(), kind=jnp.bfloat16):
    values = jax.random.normal(stream_key, shape, jnp.float32) * deviation
    if len(pieces) > 0:
        values = steps_of(stream_key, shape, pieces, -0.22, 0.18) * values
    return jnp.clip(values, min=-reach, max=reach).astype(kind)


def setup_inputs(seed: int = 0) -> dict:
    keys = jax.random.split(jax.random.key(seed), 7)
    return {
        "left_derivatives": normal_values(keys[0], (BUNDLE_TOTAL, MEASURE_ROWS, BLOCK_PARAMS), (0.4 / (BLOCK_PARAMS * MEASURE_ROWS) ** 0.25), 0.25, ((0, 128),)),
        "right_derivatives": normal_values(keys[1], (BUNDLE_TOTAL, MEASURE_ROWS, BLOCK_PARAMS), (0.4 / (BLOCK_PARAMS * MEASURE_ROWS) ** 0.25), 0.25, ((0, 128),)),
        "bundle_tile_slot": draw_bundle_tile_slot(jax.random.fold_in(keys[6], 71), 0),
        "tile_pos": draw_tile_pos(jax.random.fold_in(keys[6], 71), 0),
        "right_sides": normal_values(keys[4], (NRHS, ORDER), 1.0, 6.0, ((1, 128),), jnp.float32),
        "diagonal": jnp.clip(jnp.exp(math.log(3.0) - 1.3217558 * jax.random.uniform(keys[5], (ORDER,), jnp.float32) ** steps_of(keys[5], (ORDER,), ((0, 128),), -0.2, 0.2)), 0.8, 3.0),
    }


highest = lax.Precision.HIGHEST

def build_matrix(left_derivatives, right_derivatives, bundle_tile_slot):
    slot_total = N_ROW * N_COL * CAP

    def add_bundle(matrix, bundle):
        left_panel, right_panel, target = bundle
        product = jnp.dot(left_panel.T, right_panel, preferred_element_type=jnp.float32).astype(jnp.bfloat16)
        product = lax.optimization_barrier(product).astype(jnp.float32)
        return (matrix.at[target].add(product), None)
    empty = jnp.zeros((slot_total, BLOCK_PARAMS, BLOCK_PARAMS), jnp.float32)
    matrix, ignored = lax.scan(add_bundle, empty, (left_derivatives, right_derivatives, bundle_tile_slot.astype(jnp.int32)))
    return matrix

def block_places(tile_pos):
    slot_index = jnp.arange(N_ROW * N_COL * CAP, dtype=jnp.int32)
    device = slot_index // CAP
    position = tile_pos.reshape(-1).astype(jnp.int32)
    column_span = N_ROW * BLK_DEV
    local_column = position % column_span
    block_rows = device // N_COL * N_COL * BLK_DEV + position // column_span
    block_cols = (local_column // BLK_DEV * N_COL + device % N_COL) * BLK_DEV + local_column % BLK_DEV
    return (block_rows.astype(jnp.int32), block_cols.astype(jnp.int32))

def operate(vector, matrix, block_rows, block_cols, diagonal):
    blocks = vector.reshape(NRHS, BLOCKS, BLOCK_PARAMS)

    def visit(totals, slot_data):
        one_tile, row_block, col_block = slot_data
        from_cols = lax.dynamic_index_in_dim(blocks, col_block, 1, keepdims=False)
        from_rows = lax.dynamic_index_in_dim(blocks, row_block, 1, keepdims=False)
        totals = totals.at[:, row_block].add(jnp.dot(from_cols, one_tile.T, precision=highest))
        totals = totals.at[:, col_block].add(jnp.dot(from_rows, one_tile, precision=highest))
        return (totals, None)
    totals, ignored = lax.scan(visit, jnp.zeros_like(blocks), (matrix, block_rows, block_cols))
    return totals.reshape(NRHS, -1) + diagonal[None, :] * vector

def inner(first_side, second_side):
    return lax.optimization_barrier(jnp.sum(first_side * second_side, axis=1))

def reference(left_derivatives, right_derivatives, bundle_tile_slot, tile_pos, right_sides, diagonal):
    matrix = build_matrix(left_derivatives, right_derivatives, bundle_tile_slot)
    block_rows, block_cols = block_places(tile_pos)
    count_rhs = right_sides.shape[0]
    beta_now = jnp.sqrt(inner(right_sides, right_sides))
    beta_old = jnp.zeros((count_rhs,), jnp.float32)
    lanczos_old = right_sides
    lanczos_now = right_sides
    delta_bar = jnp.zeros((count_rhs,), jnp.float32)
    epsilon_now = jnp.zeros((count_rhs,), jnp.float32)
    phi_bar = beta_now
    cosine = -jnp.ones((count_rhs,), jnp.float32)
    sine_now = jnp.zeros((count_rhs,), jnp.float32)
    search_now = jnp.zeros_like(right_sides)
    search_old = jnp.zeros_like(right_sides)
    solution = jnp.zeros_like(right_sides)
    for iteration in range(ITERS):
        basis = lanczos_now / beta_now[:, None]
        image = operate(basis, matrix, block_rows, block_cols, diagonal)
        if iteration > 0:
            image = image - (beta_now / beta_old)[:, None] * lanczos_old
        alpha_now = inner(basis, image)
        image = image - (alpha_now / beta_now)[:, None] * lanczos_now
        lanczos_old, lanczos_now = (lanczos_now, image)
        beta_old, beta_now = (beta_now, jnp.sqrt(inner(image, image)))
        epsilon_old = epsilon_now
        delta_now = cosine * delta_bar + sine_now * alpha_now
        gamma_bar = sine_now * delta_bar - cosine * alpha_now
        epsilon_now = sine_now * beta_now
        delta_bar = -cosine * beta_now
        gamma_now = jnp.sqrt(gamma_bar * gamma_bar + beta_now * beta_now)
        cosine = gamma_bar / gamma_now
        sine_now = beta_now / gamma_now
        phi_now = cosine * phi_bar
        phi_bar = sine_now * phi_bar
        search_older, search_old = (search_old, search_now)
        search_now = (basis - epsilon_old[:, None] * search_older - delta_now[:, None] * search_old) / gamma_now[:, None]
        solution = solution + phi_now[:, None] * search_now
    return solution
```

```python
import jax
import jax.numpy as jnp
from jax import lax
from jax.experimental import pallas as pl
from jax.experimental.pallas import tpu as pltpu
from jax.sharding import Mesh
from jax.sharding import PartitionSpec as P

BLOCK_PARAMS = 512
NRHS = 16
BLK_DEV = 4
CAP = 16
SEND_CAP = 2
N_Y = 4
N_CORE = 2
N_ROW = 8
N_COL = 16
BUN_DEV = 8
BAND = N_COL * BLK_DEV
SPAN = N_ROW * BLK_DEV
MSG = BLK_DEV + 1
COL = ("col_0", "col_1")
ROW = ("row_0", "row_1")
ROW_COL = ("row_0", "row_1", "col_0", "col_1")
bf16 = jnp.bfloat16
f32 = jnp.float32


def select_kernel(index_ref, view_ref, out_ref):
    for slot in range(N_COL * SEND_CAP):
        out_ref[slot] = view_ref[index_ref[slot]]


def select_blocks(index, view):
    return pl.pallas_call(
        select_kernel,
        out_shape=jax.ShapeDtypeStruct((N_COL * SEND_CAP, NRHS, BLOCK_PARAMS), bf16),
        in_specs=[
            pl.BlockSpec(memory_space=pltpu.SMEM),
            pl.BlockSpec(memory_space=pltpu.VMEM),
        ],
        out_specs=pl.BlockSpec(memory_space=pltpu.VMEM),
    )(index, view)


def across_kernel(row_ref, view_ref, gram_ref, out_ref):
    for bundle in range(BUN_DEV):
        out_ref[bundle] = jnp.dot(
            view_ref[row_ref[bundle]], gram_ref[bundle], preferred_element_type=f32
        ).astype(bf16)


def across_products(row_place, band_view, grams):
    return pl.pallas_call(
        across_kernel,
        out_shape=jax.ShapeDtypeStruct((BUN_DEV, NRHS, BLOCK_PARAMS), bf16),
        in_specs=[
            pl.BlockSpec(memory_space=pltpu.SMEM),
            pl.BlockSpec(memory_space=pltpu.VMEM),
            pl.BlockSpec(memory_space=pltpu.VMEM),
        ],
        out_specs=pl.BlockSpec(memory_space=pltpu.VMEM),
    )(row_place, band_view, grams)


def band_kernel(row_ref, slot_ref, label_ref, taken_ref, arrived_ref, gram_ref, out_ref, total_ref):
    total_ref[...] = jnp.zeros_like(total_ref)
    for bundle in range(BUN_DEV):
        product = lax.dot_general(
            taken_ref[slot_ref[bundle]],
            gram_ref[bundle],
            (((1,), (1,)), ((), ())),
            preferred_element_type=f32,
        )
        total_ref[row_ref[bundle]] += product

    def add_arrived(item, carry):
        label = label_ref[item]

        @pl.when(label >= 0)
        def _():
            total_ref[label] += arrived_ref[item].astype(f32)

        return carry

    lax.fori_loop(0, N_ROW * BUN_DEV, add_arrived, 0)
    out_ref[...] = total_ref[...].astype(bf16)


def band_sums(row_place, slot_place, labels, taken, arrived, grams):
    return pl.pallas_call(
        band_kernel,
        out_shape=jax.ShapeDtypeStruct((BAND, NRHS, BLOCK_PARAMS), bf16),
        in_specs=[pl.BlockSpec(memory_space=pltpu.SMEM)] * 3
        + [pl.BlockSpec(memory_space=pltpu.VMEM)] * 3,
        out_specs=pl.BlockSpec(memory_space=pltpu.VMEM),
        scratch_shapes=[pltpu.VMEM((BAND, NRHS, BLOCK_PARAMS), f32)],
    )(row_place, slot_place, labels, taken, arrived, grams)


def from_behind(shard, axis):
    size = lax.axis_size(axis)
    pieces = [shard]
    for step in range(1, size):
        pieces.append(lax.ppermute(shard, axis, [(i, (i + step) % size) for i in range(size)]))
    return jnp.stack(pieces)


def over_row(shard):
    chips = from_behind(shard, "row_0")
    return from_behind(chips, "row_1")


def over_col(shard):
    ring = from_behind(shard, "col_0")
    return from_behind(ring, "col_1")


def swapped(blocks):
    return lax.all_to_all(blocks, COL, split_axis=0, concat_axis=0, tiled=True)


def total_over_col(partial):
    partial = jnp.sum(from_behind(partial, "col_0"), axis=0)
    return jnp.sum(from_behind(partial, "col_1"), axis=0)


def split_pieces(sums):
    high = lax.reduce_precision(sums, 8, 7)
    rest = sums - high
    middle = lax.reduce_precision(rest, 8, 7)
    low = rest - middle
    return jnp.concatenate([high, middle, low], axis=1).astype(bf16)


def joined_pieces(pieces, count):
    pieces = pieces.astype(f32)
    parts = pieces.reshape(pieces.shape[:-1] + (3, count))
    return parts[..., 0, :] + parts[..., 1, :] + parts[..., 2, :]


def routes(bundle_tile_slot, tile_pos):
    y, core = lax.axis_index("row_0"), lax.axis_index("row_1")
    z, x = lax.axis_index("col_0"), lax.axis_index("col_1")
    my_col, my_row = z * 4 + x, y * N_CORE + core
    own_pos = tile_pos.reshape(CAP)
    packed = jnp.concatenate([own_pos, bundle_tile_slot, jnp.zeros((104,), jnp.int32)])
    table = over_col(packed.reshape(1, 128)).reshape(N_COL, 128)
    step_x = jnp.arange(N_COL, dtype=jnp.int32) // 4
    step_z = jnp.arange(N_COL, dtype=jnp.int32) % 4
    source_col = (z - step_z + 4) % 4 * 4 + (x - step_x + 4) % 4
    serial = jnp.arange(BUN_DEV, dtype=jnp.int32)
    earlier = serial[None, :] < serial[:, None]
    entry = jnp.arange(CAP, dtype=jnp.int32)

    owner = bundle_tile_slot // CAP % N_COL
    within = bundle_tile_slot % CAP
    same = jnp.logical_and(owner[:, None] == owner[None, :], earlier)
    rank = jnp.sum(same.astype(jnp.int32), axis=1)
    hit = jnp.logical_and(
        (owner[:, None] == source_col[None, :])[:, :, None],
        (within[:, None] == entry[None, :])[:, None, :],
    )
    position = jnp.sum(jnp.where(hit, table[None, :, :CAP], 0), axis=(1, 2))
    row_place = position // SPAN
    across = position % SPAN
    slot_place = owner * SEND_CAP + rank
    label = across // BLK_DEV * BAND + owner * BLK_DEV + across % BLK_DEV

    asked = table[:, CAP : CAP + BUN_DEV]
    asked_here = asked // CAP % N_COL == my_col
    before = jnp.logical_and(asked_here[:, None, :], earlier[None])
    asked_rank = jnp.sum(before.astype(jnp.int32), axis=2)
    asked_hit = asked[:, :, None] % CAP == entry[None, None, :]
    asked_across = jnp.sum(jnp.where(asked_hit, own_pos[None, None, :], 0), axis=2) % SPAN
    numbered = jnp.logical_and(
        asked_here[:, :, None],
        asked_rank[:, :, None] == jnp.arange(SEND_CAP, dtype=jnp.int32)[None, None, :],
    )
    wanted = jnp.sum(jnp.where(numbered, asked_across[:, :, None], 0), axis=1)
    ordered = source_col[None, :] == jnp.arange(N_COL, dtype=jnp.int32)[:, None]
    wanted = jnp.sum(jnp.where(ordered[:, :, None], wanted[None], 0), axis=1).reshape(-1)
    wanted_row = wanted // BLK_DEV
    step_core = (wanted_row % N_CORE - core) % N_CORE
    step_y = (y - wanted_row // N_CORE + N_Y) % N_Y
    send_index = (step_core * N_Y + step_y) * MSG + wanted % BLK_DEV

    labels = over_row(jnp.pad(label, (0, 120)).reshape(1, 128))
    labels = labels.reshape(N_ROW, 128)[:, :BUN_DEV].reshape(-1)
    labels = jnp.where(labels // BAND == my_row, labels % BAND, -1)
    return row_place, slot_place, send_index, labels


def body(left_derivatives, right_derivatives, bundle_tile_slot, tile_pos, right_sides, diagonal):
    row_place, slot_place, send_index, labels = routes(bundle_tile_slot, tile_pos)
    grams = jnp.einsum(
        "nma,nmb->nab", left_derivatives, right_derivatives, preferred_element_type=f32
    ).astype(bf16)
    initial = right_sides.reshape(NRHS, BLK_DEV, BLOCK_PARAMS).transpose(1, 0, 2)
    weight = diagonal.reshape(BLK_DEV, 1, BLOCK_PARAMS)

    def wide(scalar):
        return scalar[None, :, None]

    def dots(pairs):
        return jnp.stack([jnp.sum(first * second, axis=(0, 2)) for first, second in pairs], axis=1)

    def operate(vector, sums):
        count = sums.shape[1]
        sent = vector.astype(bf16)
        band_view = swapped(jnp.broadcast_to(sent, (N_COL,) + sent.shape))
        band_view = band_view.reshape(BAND, NRHS, BLOCK_PARAMS)
        extra = jnp.pad(split_pieces(sums), ((0, 0), (0, BLOCK_PARAMS - 3 * count)))
        view = over_row(jnp.concatenate([sent, extra[None]], axis=0))
        view = view.reshape(N_ROW, MSG, NRHS, BLOCK_PARAMS)
        in_row = jnp.sum(joined_pieces(view[:, BLK_DEV, :, : 3 * count], count), axis=0)
        everywhere = total_over_col(in_row)
        picked = select_blocks(send_index, view.reshape(N_ROW * MSG, NRHS, BLOCK_PARAMS))
        taken = swapped(picked.reshape(N_COL, SEND_CAP, NRHS, BLOCK_PARAMS))
        across = across_products(row_place, band_view, grams)
        arrived = over_row(across)
        parts = band_sums(
            row_place,
            slot_place,
            labels,
            taken.reshape(N_COL * SEND_CAP, NRHS, BLOCK_PARAMS),
            arrived.reshape(N_ROW * BUN_DEV, NRHS, BLOCK_PARAMS),
            grams,
        )
        arrived_parts = swapped(parts.reshape(N_COL, BLK_DEV, NRHS, BLOCK_PARAMS))
        image = jnp.sum(arrived_parts.astype(f32), axis=0) + weight * vector
        return image, [everywhere[:, i] for i in range(count)]

    def root(value):
        return jnp.sqrt(jnp.maximum(value, 0.0))

    image, (square, weighted) = operate(initial, dots([(initial, initial), (initial, weight * initial)]))
    beta_1 = jnp.sqrt(square)
    shift = weighted / square
    first = initial / wide(beta_1)
    first_image = image / wide(beta_1)
    trial = first_image - wide(shift) * first

    image, (along, square, weighted) = operate(
        trial, dots([(first, trial), (trial, trial), (trial, weight * trial)])
    )
    alpha_1 = shift + along
    beta_2 = root(square - along * along)
    second = (trial - wide(along) * first) / wide(beta_2)
    second_image = (image - wide(along) * first_image) / wide(beta_2)
    shift = weighted / square
    trial = second_image - wide(shift) * second - wide(beta_2) * first

    image, (along, square) = operate(trial, dots([(second, trial), (trial, trial)]))
    alpha_2 = shift + along
    beta_3 = root(square - along * along)
    third = (trial - wide(along) * second) / wide(beta_3)
    third_image = (image - wide(along) * second_image) / wide(beta_3)
    shift = alpha_2
    trial = third_image - wide(shift) * third - wide(beta_3) * second

    sums = dots([(third, trial), (trial, trial)])
    sums = jnp.pad(sums.T.reshape(1, 2 * NRHS), ((0, 0), (0, 128 - 2 * NRHS)))
    sums = lax.all_to_all(
        jnp.broadcast_to(sums, (N_ROW * N_COL, 1, 128)), ROW_COL, split_axis=0, concat_axis=0, tiled=True
    )
    sums = jnp.sum(sums, axis=(0, 1))
    along, square = sums[:NRHS], sums[NRHS : 2 * NRHS]
    alpha_3 = shift + along
    beta_4 = root(square - along * along)

    delta_bar = jnp.zeros_like(beta_1)
    epsilon_now = jnp.zeros_like(beta_1)
    phi_bar = beta_1
    cosine = -jnp.ones_like(beta_1)
    sine_now = jnp.zeros_like(beta_1)
    search_now = jnp.zeros_like(first)
    search_old = jnp.zeros_like(first)
    solution = jnp.zeros_like(first)
    for basis, alpha_now, beta_now in (
        (first, alpha_1, beta_2),
        (second, alpha_2, beta_3),
        (third, alpha_3, beta_4),
    ):
        epsilon_old = epsilon_now
        delta_now = cosine * delta_bar + sine_now * alpha_now
        gamma_bar = sine_now * delta_bar - cosine * alpha_now
        epsilon_now = sine_now * beta_now
        delta_bar = -cosine * beta_now
        gamma_now = jnp.sqrt(gamma_bar * gamma_bar + beta_now * beta_now)
        cosine = gamma_bar / gamma_now
        sine_now = beta_now / gamma_now
        phi_now = cosine * phi_bar
        phi_bar = sine_now * phi_bar
        search_older, search_old = (search_old, search_now)
        search_now = (
            basis - wide(epsilon_old) * search_older - wide(delta_now) * search_old
        ) / wide(gamma_now)
        solution = solution + wide(phi_now) * search_now
    return solution.transpose(1, 0, 2).reshape(NRHS, BLK_DEV * BLOCK_PARAMS)


def solution(mesh):
    torus = Mesh(mesh.devices.reshape(4, 2, 4, 4), ("row_0", "row_1", "col_0", "col_1"))
    return jax.shard_map(
        body,
        mesh=torus,
        in_specs=(
            P(ROW_COL, None, None),
            P(ROW_COL, None, None),
            P(ROW_COL),
            P(ROW, COL, None),
            P(None, ROW_COL),
            P(ROW_COL),
        ),
        out_specs=P(None, ROW_COL),
        check_vma=False,
    )
```
